32 devices in a mesh: dp: 4 (over x, y), sp: 8 (over z, core).
Axes of the slice: x: 2, y: 2, z: 4, core: 2. Of those that a mesh axis runs over, the one named last changes fastest.
Arguments:
- x_special: bfloat16 [64, 1, 1024], P('dp'), parts along dimension 0
- x_patch: bfloat16 [64, 512, 1024], P('dp', 'sp'), parts along dimension 0
- dy_special: bfloat16 [64, 1, 1024], P('dp'), parts along dimension 0
- dy_patch: bfloat16 [64, 512, 1024], P('dp', 'sp'), parts along dimension 0
- ln_scale: float32 [1024], replicated
- ln_bias: float32 [1024], replicated
- w_qkv: bfloat16 [1024, 3072], replicated
- b_qkv: float32 [3072], replicated
- w_proj: bfloat16 [1024, 1024], replicated
- b_proj: float32 [1024], replicated
- layer_scale: float32 [1024], replicated
Outputs:
- output 1: bfloat16 [64, 1, 1024], P('dp'), parts along dimension 0
- output 2: bfloat16 [64, 512, 1024], P('dp', 'sp'), parts along dimension 0
- output 3: bfloat16 [64, 1, 1024], P('dp'), parts along dimension 0
- output 4: bfloat16 [64, 512, 1024], P('dp', 'sp'), parts along dimension 0
- output 5: float32 [4096], P('dp'), parts along dimension 0
- output 6: float32 [4096], P('dp'), parts along dimension 0
- output 7: float32 [4096, 3072], P('dp'), parts along dimension 0
- output 8: float32 [12288], P('dp'), parts along dimension 0
- output 9: float32 [4096, 1024], P('dp'), parts along dimension 0
- output 10: float32 [4096], P('dp'), parts along dimension 0
- output 11: float32 [4096], P('dp'), parts along dimension 0
There are 4 independent parts. The reference program is written for one: setup_inputs(seed, part) draws one part's arguments, and reference() takes and returns one part's arrays. A program takes and returns all parts, laid end to end along the dimension named above; an argument that names none is the same for every part.
All inputs are finite; a program needn't handle non-finite values.
Results may differ from the reference program's by a relative error of at most 0.01016.
Values are sent between devices in bfloat16 or wider.
A program may use at most 1 GiB of HBM per device.

```python
import jax
import jax.numpy as jnp
from jax import lax

IMAGES = 16
PATCHES = 512
SPECIAL = 1
D_MODEL = 1024
NUM_HEADS = 16
HEAD_DIM = 64
TEXTURES = 8
TOKENS = SPECIAL + PATCHES
LN_EPS = 1e-6
ATTN_SCALE = HEAD_DIM ** -0.5


def setup_inputs(seed: int = 0, part: int = 0) -> dict:
    part_keys = jax.random.split(jax.random.fold_in(jax.random.key(seed), part), 7)
    weight_keys = jax.random.split(jax.random.key(seed + 1), 9)
    common = jax.random.normal(part_keys[0], (IMAGES, 1, D_MODEL), jnp.float32)
    texture = jax.random.normal(part_keys[1], (IMAGES, TEXTURES, D_MODEL), jnp.float32)
    tex_id = jax.random.randint(part_keys[2], (IMAGES, PATCHES), 0, TEXTURES)
    onehot = (tex_id[:, :, None] == jnp.arange(TEXTURES)[None, None, :]).astype(jnp.float32)
    patch_vals = jnp.einsum('bnt,btd->bnd', onehot, texture) + 0.7 * common + 0.5 * jax.random.normal(part_keys[3], (IMAGES, PATCHES, D_MODEL), jnp.float32)
    special_vals = 3.0 * common + 0.5 * jax.random.normal(part_keys[4], (IMAGES, SPECIAL, D_MODEL), jnp.float32)
    dy_special = jax.random.normal(part_keys[5], (IMAGES, SPECIAL, D_MODEL), jnp.float32)
    dy_patch = jax.random.normal(part_keys[6], (IMAGES, PATCHES, D_MODEL), jnp.float32)
    fan_scale = D_MODEL ** -0.5
    w_query = jax.random.normal(weight_keys[0], (D_MODEL, D_MODEL), jnp.float32)
    w_key = 0.6 * w_query + 0.8 * jax.random.normal(weight_keys[1], (D_MODEL, D_MODEL), jnp.float32)
    w_value = jax.random.normal(weight_keys[2], (D_MODEL, D_MODEL), jnp.float32)
    w_qkv = jnp.concatenate([w_query, w_key, w_value], axis=1) * fan_scale
    w_proj = jax.random.normal(weight_keys[3], (D_MODEL, D_MODEL), jnp.float32) * fan_scale
    return {
        'x_special': special_vals.astype(jnp.bfloat16),
        'x_patch': patch_vals.astype(jnp.bfloat16),
        'dy_special': dy_special.astype(jnp.bfloat16),
        'dy_patch': dy_patch.astype(jnp.bfloat16),
        'ln_scale': 1.0 + 0.2 * jax.random.normal(weight_keys[4], (D_MODEL,), jnp.float32),
        'ln_bias': 0.3 * jax.random.normal(weight_keys[5], (D_MODEL,), jnp.float32),
        'w_qkv': w_qkv.astype(jnp.bfloat16),
        'b_qkv': 0.3 * jax.random.normal(weight_keys[6], (3 * D_MODEL,), jnp.float32),
        'w_proj': w_proj.astype(jnp.bfloat16),
        'b_proj': 0.3 * jax.random.normal(weight_keys[7], (D_MODEL,), jnp.float32),
        'layer_scale': jax.random.uniform(weight_keys[8], (D_MODEL,), jnp.float32, 0.4, 1.2),
    }


def head_attention(head_qkv):
    queries = head_qkv[0].astype(jnp.float32)
    key_rows = head_qkv[1].astype(jnp.float32)
    value_rows = head_qkv[2].astype(jnp.float32)
    scores = jnp.dot(queries, key_rows.T) * ATTN_SCALE
    attn_prob = jax.nn.softmax(scores, axis=-1)
    return jnp.dot(attn_prob.astype(jnp.bfloat16).astype(jnp.float32), value_rows).astype(jnp.bfloat16)


def block_forward(x_all, ln_scale, ln_bias, w_qkv, b_qkv, w_proj, b_proj, layer_scale):
    x_float = x_all.astype(jnp.float32)
    centered = x_float - jnp.mean(x_float, axis=-1, keepdims=True)
    inv_std = lax.rsqrt(jnp.mean(centered * centered, axis=-1, keepdims=True) + LN_EPS)
    normed = (centered * inv_std * ln_scale + ln_bias).astype(jnp.bfloat16)
    qkv_rows = jnp.einsum('btd,de->bte', normed.astype(jnp.float32), w_qkv.astype(jnp.float32)) + b_qkv
    qkv_rows = qkv_rows.astype(jnp.bfloat16).reshape(IMAGES, TOKENS, 3, NUM_HEADS, HEAD_DIM)
    per_head = jnp.transpose(qkv_rows, (0, 3, 2, 1, 4)).reshape(IMAGES * NUM_HEADS, 3, TOKENS, HEAD_DIM)
    attn_out = lax.map(jax.checkpoint(head_attention), per_head)
    attn_out = jnp.transpose(attn_out.reshape(IMAGES, NUM_HEADS, TOKENS, HEAD_DIM), (0, 2, 1, 3)).reshape(IMAGES, TOKENS, D_MODEL)
    proj_out = jnp.einsum('btd,de->bte', attn_out.astype(jnp.float32), w_proj.astype(jnp.float32)) + b_proj
    return (x_float + layer_scale * proj_out).astype(jnp.bfloat16)


def reference(x_special, x_patch, dy_special, dy_patch, ln_scale, ln_bias, w_qkv, b_qkv, w_proj, b_proj, layer_scale):
    x_all = jnp.concatenate([x_special, x_patch], axis=1)
    dy_all = jnp.concatenate([dy_special, dy_patch], axis=1)
    out_all, block_vjp = jax.vjp(block_forward, x_all, ln_scale, ln_bias, w_qkv, b_qkv, w_proj, b_proj, layer_scale)
    grad_list = block_vjp(dy_all)
    dx_all = grad_list[0]
    return (out_all[:, :SPECIAL], out_all[:, SPECIAL:], dx_all[:, :SPECIAL], dx_all[:, SPECIAL:], grad_list[1], grad_list[2], grad_list[3].astype(jnp.float32), grad_list[4], grad_list[5].astype(jnp.float32), grad_list[6], grad_list[7])
```

```python
import functools

import jax
import jax.numpy as jnp
from jax import lax
from jax.experimental import pallas as pl
from jax.experimental.pallas import tpu as pltpu
from jax.sharding import PartitionSpec as P

HEAD_DIM = 64
LN_EPS = 1e-6
ATTN_SCALE = HEAD_DIM ** -0.5
LANES = 128
PAD = 16
CHUNK_TILES = 3
OFFSETS = (4, 3, 5, 2, 6, 1, 7)
MESH = pl.DeviceIdType.MESH
F32 = jnp.float32
BF16 = jnp.bfloat16
NEG = -1e30


def dot_nn(a, b):
    return lax.dot_general(a, b, (((1,), (0,)), ((), ())), preferred_element_type=F32)


def dot_nt(a, b):
    return lax.dot_general(a, b, (((1,), (1,)), ((), ())), preferred_element_type=F32)


def dot_tn(a, b):
    return lax.dot_general(a, b, (((0,), (0,)), ((), ())), preferred_element_type=F32)


def normalize(x):
    x = x.astype(F32)
    centered = x - jnp.mean(x, axis=-1, keepdims=True)
    inv = lax.rsqrt(jnp.mean(centered * centered, axis=-1, keepdims=True) + LN_EPS)
    return centered * inv, inv


def block_kernel(n_dev, special, x_hbm, dy_hbm, xs_ref, dys_ref, ln_s, ln_b, wq, wk, wv, bq, bk, bv, wp, b_proj, l_scale,
                 out_hbm, dx_hbm, grad_hbm, vec_hbm,
                 x_s, dy_s, h_s, dp_s, o_acc, dh_acc, q_s, k_s, v_s, da_s, a_s, dq_s, dk_s, dv_s, dwb, recv0, recv_a, recv_b, vbuf,
                 x_snd, x_rcv, dy_snd, dy_rcv, out_snd, out_rcv, dx_snd, dx_rcv, vec_snd, vec_rcv,
                 s0, r0, s_a, r_a, s_b, r_b, s_d, r_d, s_l, loc):
    step = pl.program_id(0)
    n_steps = pl.num_programs(0)
    me = lax.axis_index('sp')
    core = lax.rem(me, 2)
    chip = me // 2
    partner = me + 1 - 2 * core
    inner = (chip == 1) | (chip == 2)
    odd = lax.rem(chip, 2)
    near_a = me + 2 - 4 * odd
    near_b = lax.rem(me + 6 + 4 * odd, n_dev)
    imgs, rows, d_model = x_s.shape
    patches = rows - PAD
    loc_p = patches // n_dev
    half = dwb.shape[1] // 2
    chunk = rows // CHUNK_TILES

    def to(peer):
        return {'sp': peer}

    def remote(src, dst, snd, rcv, peer):
        return pltpu.make_async_remote_copy(src, dst, snd, rcv, device_id=to(peer), device_id_type=MESH)

    def scatter_in(src, dst, snd, rcv, d):
        peer = lax.rem(me + d, n_dev)
        return remote(src.at[pl.ds(peer * imgs, imgs)], dst.at[:, pl.ds(pl.multiple_of(me * loc_p, loc_p), loc_p)], snd.at[d], rcv.at[d], peer)

    def local_in(src, dst, sem):
        return pltpu.make_async_copy(src.at[pl.ds(me * imgs, imgs)], dst.at[:, pl.ds(pl.multiple_of(me * loc_p, loc_p), loc_p)], sem)

    def scatter_out(src, dst, snd, rcv, d):
        peer = lax.rem(me + d, n_dev)
        return remote(src.at[:, pl.ds(pl.multiple_of(peer * loc_p, loc_p), loc_p)], dst.at[pl.ds(me * imgs, imgs)], snd.at[d], rcv.at[d], peer)

    def local_out(src, dst, sem):
        return pltpu.make_async_copy(src.at[:, pl.ds(pl.multiple_of(me * loc_p, loc_p), loc_p)], dst.at[pl.ds(me * imgs, imgs)], sem)

    def vec_copy(d):
        peer = lax.rem(me + d, n_dev)
        return remote(vbuf, vec_hbm.at[me], vec_snd.at[d], vec_rcv.at[d], peer)

    def pair_copy(b):
        slot = lax.rem(b, 2)
        return remote(dwb.at[slot, pl.ds(pl.multiple_of((1 - core) * half, half), half)], recv0.at[b], s0.at[b], r0.at[b], partner)

    def up_copy(b):
        return remote(recv0.at[b], recv_a.at[b], s_a.at[b], r_a.at[b], near_a)

    def mid_copy(b):
        return remote(recv0.at[b], recv_b.at[b], s_b.at[b], r_b.at[b], near_b)

    def down_copy(b):
        return remote(recv_a.at[b], recv_a.at[b], s_a.at[b], r_a.at[b], near_a)

    def own_rows():
        return pl.ds(pl.multiple_of(core * half, half), half)

    def share_copy(b):
        return remote(recv_a.at[b], grad_hbm.at[b, own_rows()], s_d.at[b], r_d.at[b], partner)

    def keep_copy(b):
        return pltpu.make_async_copy(recv_a.at[b], grad_hbm.at[b, own_rows()], s_l.at[b])

    add_rows = half // 8

    def stage_pair(b):
        copy = pair_copy(b)
        copy.wait_recv()
        copy.wait_send()
        slot = lax.rem(b, 2)

        def body(t, carry):
            r = pl.multiple_of(t * add_rows, add_rows)
            recv0[b, pl.ds(r, add_rows)] += dwb[slot, pl.ds(pl.multiple_of(core * half + r, add_rows), add_rows)]
            return carry
        lax.fori_loop(0, 8, body, 0)

        @pl.when(jnp.logical_not(inner))
        def _():
            up_copy(b).start()

    def stage_up(b):
        up_copy(b).wait_recv()

        def body(t, carry):
            r = pl.multiple_of(t * add_rows, add_rows)
            recv0[b, pl.ds(r, add_rows)] += recv_a[b, pl.ds(r, add_rows)]
            return carry
        lax.fori_loop(0, 8, body, 0)
        mid_copy(b).start()

    def stage_mid(b):
        mid_copy(b).wait_recv()

        def body(t, carry):
            r = pl.multiple_of(t * add_rows, add_rows)
            recv_a[b, pl.ds(r, add_rows)] = recv0[b, pl.ds(r, add_rows)] + recv_b[b, pl.ds(r, add_rows)]
            return carry
        lax.fori_loop(0, 8, body, 0)
        down_copy(b).start()
        share_copy(b).start()
        keep_copy(b).start()

    def stage_down(b):
        down_copy(b).wait_recv()
        share_copy(b).start()
        keep_copy(b).start()

    def advance(g):
        @pl.when(jnp.logical_not(inner) & (g >= 3))
        def _():
            stage_down(g - 3)

        @pl.when(inner & (g >= 2) & (g < n_steps + 2))
        def _():
            stage_mid(g - 2)

        @pl.when(inner & (g >= 1) & (g < n_steps + 1))
        def _():
            stage_up(g - 1)

    @pl.when(step == 0)
    def _():
        barrier = pltpu.get_barrier_semaphore()
        for d in OFFSETS:
            pl.semaphore_signal(barrier, inc=1, device_id=to(lax.rem(me + d, n_dev)), device_id_type=MESH)
        pl.semaphore_wait(barrier, n_dev - 1)
        for d in OFFSETS:
            scatter_in(x_hbm, x_s, x_snd, x_rcv, d).start()
        for d in OFFSETS:
            scatter_in(dy_hbm, dy_s, dy_snd, dy_rcv, d).start()
        local_in(x_hbm, x_s, loc.at[0]).start()
        local_in(dy_hbm, dy_s, loc.at[1]).start()
        for i in range(imgs):
            x_s[i, patches:] = xs_ref[i]
            dy_s[i, patches:] = dys_ref[i]
        vbuf[...] = jnp.zeros_like(vbuf)
        local_in(x_hbm, x_s, loc.at[0]).wait()
        for d in OFFSETS:
            scatter_in(x_hbm, x_s, x_snd, x_rcv, d).wait_recv()

        def ln_body(t, carry):
            i, r = t // CHUNK_TILES, pl.multiple_of(lax.rem(t, CHUNK_TILES) * chunk, 16)
            x_hat, _ = normalize(x_s[i, pl.ds(r, chunk)])
            h_s[i, pl.ds(r, chunk)] = (x_hat * ln_s[...] + ln_b[...]).astype(BF16)
            o_acc[i, pl.ds(r, chunk)] = jnp.zeros((chunk, d_model), F32)
            dh_acc[i, pl.ds(r, chunk)] = jnp.zeros((chunk, d_model), F32)
            return carry
        lax.fori_loop(0, imgs * CHUNK_TILES, ln_body, 0)
        local_in(dy_hbm, dy_s, loc.at[1]).wait()
        for d in OFFSETS:
            scatter_in(dy_hbm, dy_s, dy_snd, dy_rcv, d).wait_recv()

        def dy_body(t, total):
            i, r = t // CHUNK_TILES, pl.multiple_of(lax.rem(t, CHUNK_TILES) * chunk, 16)
            d_proj = dy_s[i, pl.ds(r, chunk)].astype(F32) * l_scale[...]
            dp_s[i, pl.ds(r, chunk)] = d_proj.astype(BF16)
            return total + jnp.sum(d_proj, axis=0, keepdims=True)
        d_bias = lax.fori_loop(0, imgs * CHUNK_TILES, dy_body, jnp.zeros((1, d_model), F32))
        for c in range(8):
            vbuf[40 + c:41 + c] = d_bias[:, c * LANES:(c + 1) * LANES]
        for d in OFFSETS:
            scatter_in(x_hbm, x_s, x_snd, x_rcv, d).wait_send()
            scatter_in(dy_hbm, dy_s, dy_snd, dy_rcv, d).wait_send()

    def project(i, carry):
        h = h_s[i]
        q_s[i] = (dot_nn(h, wq[...]) + bq[...]).astype(BF16)
        k_s[i] = (dot_nn(h, wk[...]) + bk[...]).astype(BF16)
        v_s[i] = (dot_nn(h, wv[...]) + bv[...]).astype(BF16)
        da_s[i] = dot_nt(dp_s[i], wp[...]).astype(BF16)
        return carry
    lax.fori_loop(0, imgs, project, 0)

    lane = lax.broadcasted_iota(jnp.int32, (1, LANES), 1)
    zero = jnp.zeros((), BF16)

    def attend(i, carry):
        q, k, v, da = q_s[i], k_s[i], v_s[i], da_s[i]
        a = jnp.zeros((rows, LANES), F32)
        dq, dk, dv = a, a, a
        keep_col = lax.broadcasted_iota(jnp.int32, (1, rows), 1) < patches + special
        for t in range(LANES // HEAD_DIM):
            mine = (lane // HEAD_DIM) == t
            qm, km, vm, dam = (jnp.where(mine, y, zero) for y in (q, k, v, da))
            s = dot_nt(qm, k) * ATTN_SCALE
            s = jnp.where(keep_col, s, NEG)
            e = jnp.exp(s - jnp.max(s, axis=-1, keepdims=True))
            p = e * (1.0 / jnp.sum(e, axis=-1, keepdims=True))
            p_lo = p.astype(BF16)
            a = a + dot_nn(p_lo, vm)
            dv = dv + dot_tn(p_lo, dam)
            dp = dot_nt(dam, v).astype(BF16).astype(F32)
            ds = (p * (dp - jnp.sum(dp * p, axis=-1, keepdims=True)) * ATTN_SCALE).astype(BF16)
            dq = dq + dot_nn(ds, km)
            dk = dk + dot_tn(ds, qm)
        a_s[i] = a.astype(BF16)
        dq_s[i] = dq.astype(BF16)
        dk_s[i] = dk.astype(BF16)
        dv_s[i] = dv.astype(BF16)
        return carry
    lax.fori_loop(0, imgs, attend, 0)

    def back(i, carry):
        o_acc[i] += dot_nn(a_s[i], wp[...])
        dh_acc[i] += dot_nt(dq_s[i], wq[...]) + dot_nt(dk_s[i], wk[...]) + dot_nt(dv_s[i], wv[...])
        return carry
    lax.fori_loop(0, imgs, back, 0)

    slot = lax.rem(step, 2)
    for j, ref in enumerate((dq_s, dk_s, dv_s)):
        vbuf[pl.ds(j * 8 + step, 1)] = sum(jnp.sum(ref[i].astype(F32), axis=0, keepdims=True) for i in range(imgs))

    cols = 256

    def weight_grads(t, carry):
        c = pl.ds(pl.multiple_of(t * cols, cols), cols)
        for j, (left, right) in enumerate(((h_s, dq_s), (h_s, dk_s), (h_s, dv_s), (dp_s, a_s))):
            dwb[slot, c, j * LANES:(j + 1) * LANES] = sum(dot_tn(left[i, :, c], right[i]) for i in range(imgs))
        return carry
    lax.fori_loop(0, d_model // cols, weight_grads, 0)

    pair_copy(step).start()
    advance(step)
    stage_pair(step)

    @pl.when(step == n_steps - 1)
    def _():
        def out_body(t, total):
            i, r = t // CHUNK_TILES, pl.multiple_of(lax.rem(t, CHUNK_TILES) * chunk, 16)
            proj = o_acc[i, pl.ds(r, chunk)] + b_proj[...]
            h_s[i, pl.ds(r, chunk)] = (x_s[i, pl.ds(r, chunk)].astype(F32) + l_scale[...] * proj).astype(BF16)
            return total + jnp.sum(dy_s[i, pl.ds(r, chunk)].astype(F32) * proj, axis=0, keepdims=True)
        d_scale = lax.fori_loop(0, imgs * CHUNK_TILES, out_body, jnp.zeros((1, d_model), F32))
        for d in OFFSETS:
            scatter_out(h_s, out_hbm, out_snd, out_rcv, d).start()
        local_out(h_s, out_hbm, loc.at[2]).start()

        advance(n_steps)

        def dx_body(t, carry):
            t_scale, t_bias = carry
            i, r = t // CHUNK_TILES, pl.multiple_of(lax.rem(t, CHUNK_TILES) * chunk, 16)
            x_hat, inv = normalize(x_s[i, pl.ds(r, chunk)])
            grad = dh_acc[i, pl.ds(r, chunk)].astype(BF16).astype(F32)
            g_hat = grad * ln_s[...]
            d_row = inv * (g_hat - jnp.mean(g_hat, axis=-1, keepdims=True) - x_hat * jnp.mean(g_hat * x_hat, axis=-1, keepdims=True))
            dp_s[i, pl.ds(r, chunk)] = (dy_s[i, pl.ds(r, chunk)].astype(F32) + d_row).astype(BF16)
            return t_scale + jnp.sum(grad * x_hat, axis=0, keepdims=True), t_bias + jnp.sum(grad, axis=0, keepdims=True)
        none = jnp.zeros((1, d_model), F32)
        d_ln_s, d_ln_b = lax.fori_loop(0, imgs * CHUNK_TILES, dx_body, (none, none))
        for d in OFFSETS:
            scatter_out(dp_s, dx_hbm, dx_snd, dx_rcv, d).start()
        local_out(dp_s, dx_hbm, loc.at[3]).start()

        for c in range(8):
            part = slice(c * LANES, (c + 1) * LANES)
            vbuf[24 + c:25 + c] = d_ln_s[:, part]
            vbuf[32 + c:33 + c] = d_ln_b[:, part]
            vbuf[48 + c:49 + c] = d_scale[:, part]
            for i in range(imgs):
                vbuf[56 + 8 * i + c:57 + 8 * i + c] = h_s[i, patches:, part].astype(F32)[:1]
                vbuf[72 + 8 * i + c:73 + 8 * i + c] = dp_s[i, patches:, part].astype(F32)[:1]
        for d in OFFSETS:
            vec_copy(d).start()
        pltpu.make_async_copy(vbuf, vec_hbm.at[me], loc.at[4]).start()

        advance(n_steps + 1)
        advance(n_steps + 2)

        local_out(h_s, out_hbm, loc.at[2]).wait()
        local_out(dp_s, dx_hbm, loc.at[3]).wait()
        pltpu.make_async_copy(vbuf, vec_hbm.at[me], loc.at[4]).wait()
        for d in OFFSETS:
            scatter_out(h_s, out_hbm, out_snd, out_rcv, d).wait()
            scatter_out(dp_s, dx_hbm, dx_snd, dx_rcv, d).wait()
            vec_copy(d).wait()

        def drain(b, carry):
            up_copy(b).wait_send()

            @pl.when(inner)
            def _():
                mid_copy(b).wait_send()
            share_copy(b).wait()
            keep_copy(b).wait()
            return carry
        lax.fori_loop(0, n_steps, drain, 0)


def solution(mesh):
    n_dev = mesh.shape['sp']

    def local_block(x_special, x_patch, dy_special, dy_patch, ln_scale, ln_bias, w_qkv, b_qkv, w_proj, b_proj, layer_scale):
        num_images, special, d_model = x_special.shape
        loc_p = x_patch.shape[1]
        imgs = num_images // n_dev
        pairs = d_model // LANES
        rows = n_dev * loc_p + PAD
        me = lax.axis_index('sp')

        def own_special(arr):
            own = lax.dynamic_slice_in_dim(arr, me * imgs, imgs, axis=0)
            return jnp.pad(own, ((0, 0), (0, PAD - special), (0, 0)))

        def whole(shape):
            return pl.BlockSpec(shape, lambda g: (0,) * len(shape))

        any_spec = pl.BlockSpec(memory_space=pl.ANY)
        row = (1, d_model)
        w_specs = [pl.BlockSpec((d_model, LANES), functools.partial(lambda j, g: (0, j * pairs + g), j)) for j in range(3)]
        b_specs = [pl.BlockSpec((1, LANES), functools.partial(lambda j, g: (0, j * pairs + g), j)) for j in range(3)]
        dma = pltpu.SemaphoreType.DMA
        big = (imgs, rows, d_model)
        thin = (imgs, rows, LANES)
        half = d_model // 2
        slots = pltpu.VMEM((pairs, half, 4 * LANES), F32)
        out_p, dx_p, grads, vecs = pl.pallas_call(
            functools.partial(block_kernel, n_dev, special),
            grid=(pairs,),
            out_shape=(
                jax.ShapeDtypeStruct(x_patch.shape, BF16), jax.ShapeDtypeStruct(x_patch.shape, BF16),
                jax.ShapeDtypeStruct((pairs, d_model, 4 * LANES), F32), jax.ShapeDtypeStruct((n_dev, 88, LANES), F32)),
            in_specs=[any_spec, any_spec, whole((imgs, PAD, d_model)), whole((imgs, PAD, d_model)), whole(row), whole(row),
                      *w_specs, *b_specs, pl.BlockSpec((LANES, d_model), lambda g: (g, 0)), whole(row), whole(row)],
            out_specs=(any_spec,) * 4,
            scratch_shapes=[
                *[pltpu.VMEM(big, BF16)] * 4, *[pltpu.VMEM(big, F32)] * 2, *[pltpu.VMEM(thin, BF16)] * 8,
                pltpu.VMEM((2, d_model, 4 * LANES), F32), slots, slots, slots, pltpu.VMEM((88, LANES), F32),
                *[dma((n_dev,))] * 10, *[dma((pairs,))] * 9, dma((5,))],
            compiler_params=pltpu.CompilerParams(
                collective_id=0, has_side_effects=True, dimension_semantics=('arbitrary',), vmem_limit_bytes=67_000_000),
        )(x_patch, dy_patch, own_special(x_special), own_special(dy_special), ln_scale[None], ln_bias[None],
          w_qkv, w_qkv, w_qkv, b_qkv[None], b_qkv[None], b_qkv[None], w_proj, b_proj[None], layer_scale[None])

        d_w_qkv = jnp.transpose(grads[:, :, :3 * LANES].reshape(pairs, d_model, 3, LANES), (1, 2, 0, 3)).reshape(d_model, 3 * d_model)
        d_w_proj = jnp.transpose(grads[:, :, 3 * LANES:], (0, 2, 1)).reshape(d_model, d_model)
        sums = jnp.sum(vecs[:, :56], axis=0).reshape(7, d_model)
        lone = vecs[:, 56:].reshape(n_dev, 2, imgs, special, d_model).astype(BF16)
        out_s = lone[:, 0].reshape(x_special.shape)
        dx_s = lone[:, 1].reshape(x_special.shape)
        return (out_s, out_p, dx_s, dx_p, sums[3], sums[4], d_w_qkv, sums[:3].reshape(3 * d_model), d_w_proj, sums[5], sums[6])

    part_rows = P('dp')
    part_seq = P('dp', 'sp')
    replicated = P()
    return jax.shard_map(
        local_block, mesh=mesh,
        in_specs=(part_rows, part_seq, part_rows, part_seq, replicated, replicated, replicated, replicated, replicated, replicated, replicated),
        out_specs=(part_rows, part_seq, part_rows, part_seq, part_rows, part_rows, part_rows, part_rows, part_rows, part_rows, part_rows),
        check_vma=False)
```

```python
import functools

import jax
import jax.numpy as jnp
from jax import lax
from jax.experimental import pallas as pl
from jax.experimental.pallas import tpu as pltpu
from jax.sharding import PartitionSpec as P

HEAD_DIM = 64
LN_EPS = 1e-6
ATTN_SCALE = HEAD_DIM ** -0.5
LANES = 128
PAD = 16
CHUNK_TILES = 3
SUBS = 2
MID_LAG = 2
DOWN_LAG = 4
OFFSETS = (4, 3, 5, 2, 6, 1, 7)
MESH = pl.DeviceIdType.MESH
F32 = jnp.float32
BF16 = jnp.bfloat16
NEG = -1e30


def dot_nn(a, b):
    return lax.dot_general(a, b, (((1,), (0,)), ((), ())), preferred_element_type=F32)


def dot_nt(a, b):
    return lax.dot_general(a, b, (((1,), (1,)), ((), ())), preferred_element_type=F32)


def dot_tn(a, b):
    return lax.dot_general(a, b, (((0,), (0,)), ((), ())), preferred_element_type=F32)


def normalize(x):
    x = x.astype(F32)
    centered = x - jnp.mean(x, axis=-1, keepdims=True)
    inv = lax.rsqrt(jnp.mean(centered * centered, axis=-1, keepdims=True) + LN_EPS)
    return centered * inv, inv


def block_kernel(n_dev, special, x_hbm, dy_hbm, xs_ref, dys_ref, ln_s, ln_b, wq, wk, wv, bq, bk, bv, wp, b_proj, l_scale,
                 out_hbm, dx_hbm, dwq_hbm, dwp_hbm, vec_hbm,
                 x_s, dy_s, h_s, dp_s, o_acc, dh_acc, w_s, qkv_s, g_s, da_s, a_s, dwb, recv0, recv_a, recv_b, vbuf,
                 x_snd, x_rcv, dy_snd, dy_rcv, out_snd, out_rcv, dx_snd, dx_rcv, vec_snd, vec_rcv,
                 s0, r0, s_a, r_a, s_b, r_b, s_d, r_d, s_l, loc):
    step = pl.program_id(0)
    n_steps = pl.num_programs(0)
    me = lax.axis_index('sp')
    core = lax.rem(me, 2)
    chip = me // 2
    partner = me + 1 - 2 * core
    inner = (chip == 1) | (chip == 2)
    odd = lax.rem(chip, 2)
    near_a = me + 2 - 4 * odd
    near_b = lax.rem(me + 6 + 4 * odd, n_dev)
    imgs, rows, d_model = x_s.shape
    patches = rows - PAD
    loc_p = patches // n_dev
    sub = dwb.shape[2]
    n_sub = SUBS * n_steps
    chunk = rows // CHUNK_TILES

    def to(peer):
        return {'sp': peer}

    def remote(src, dst, snd, rcv, peer):
        return pltpu.make_async_remote_copy(src, dst, snd, rcv, device_id=to(peer), device_id_type=MESH)

    def scatter_in(src, dst, snd, rcv, i, d):
        peer = lax.rem(me + d, n_dev)
        return remote(src.at[peer * imgs + i], dst.at[i, pl.ds(pl.multiple_of(me * loc_p, loc_p), loc_p)], snd.at[i, d], rcv.at[i, d], peer)

    def local_in(src, dst, snd, i):
        return pltpu.make_async_copy(src.at[me * imgs + i], dst.at[i, pl.ds(pl.multiple_of(me * loc_p, loc_p), loc_p)], snd.at[i, 0])

    def scatter_out(src, dst, snd, rcv, d):
        peer = lax.rem(me + d, n_dev)
        return remote(src.at[:, pl.ds(pl.multiple_of(peer * loc_p, loc_p), loc_p)], dst.at[pl.ds(me * imgs, imgs)], snd.at[d], rcv.at[d], peer)

    def local_out(src, dst, sem):
        return pltpu.make_async_copy(src.at[:, pl.ds(pl.multiple_of(me * loc_p, loc_p), loc_p)], dst.at[pl.ds(me * imgs, imgs)], sem)

    def vec_copy(d):
        peer = lax.rem(me + d, n_dev)
        return remote(vbuf, vec_hbm.at[me], vec_snd.at[d], vec_rcv.at[d], peer)

    def pair_copy(g):
        return remote(dwb.at[lax.rem(g, 2), pl.ds(SUBS * (1 - core), SUBS)], recv0.at[pl.ds(SUBS * g, SUBS)], s0.at[g], r0.at[g], partner)

    def up_copy(b):
        return remote(recv0.at[b], recv_a.at[b], s_a.at[b], r_a.at[b], near_a)

    def mid_copy(b):
        return remote(recv0.at[b], recv_b.at[b], s_b.at[b], r_b.at[b], near_b)

    def down_copy(b):
        return remote(recv_a.at[b], recv_a.at[b], s_a.at[b], r_a.at[b], near_a)

    def results(b):
        r = pl.ds(pl.multiple_of((SUBS * core + lax.rem(b, SUBS)) * sub, sub), sub)
        col = (b // SUBS) * LANES
        for j in range(4):
            src = recv_a.at[b, :, pl.ds(j * LANES, LANES)]
            c = pl.ds(pl.multiple_of(col + (j * d_model if j < 3 else 0), LANES), LANES)
            yield j, src, (dwq_hbm if j < 3 else dwp_hbm).at[r, c]

    def share_copies(b):
        return [remote(src, dst, s_d.at[b, j], r_d.at[b, j], partner) for j, src, dst in results(b)]

    def keep_copies(b):
        return [pltpu.make_async_copy(src, dst, s_l.at[b, j]) for j, src, dst in results(b)]

    def publish(b):
        for copy in share_copies(b) + keep_copies(b):
            copy.start()

    parts = 4
    add_rows = sub // parts

    def add_loop(add):
        def body(t, carry):
            add(pl.ds(pl.multiple_of(t * add_rows, add_rows), add_rows))
            return carry
        lax.fori_loop(0, parts, body, 0)

    def stage_pair(g):
        copy = pair_copy(g)
        copy.wait_recv()
        copy.wait_send()

        def one(t, carry):
            b = SUBS * g + t

            def add(r):
                recv0[b, r] += dwb[lax.rem(g, 2), SUBS * core + t, r]
            add_loop(add)

            @pl.when(jnp.logical_not(inner))
            def _():
                up_copy(b).start()
            return carry
        lax.fori_loop(0, SUBS, one, 0)

    def stage_up(b):
        up_copy(b).wait_recv()

        def add(r):
            recv0[b, r] += recv_a[b, r]
        add_loop(add)
        mid_copy(b).start()

    def stage_mid(b):
        mid_copy(b).wait_recv()

        def add(r):
            recv_a[b, r] = recv0[b, r] + recv_b[b, r]
        add_loop(add)
        down_copy(b).start()
        publish(b)

    def stage_down(b):
        down_copy(b).wait_recv()
        publish(b)

    def tick(t):
        @pl.when(inner & (t < n_sub))
        def _():
            stage_up(t)

        @pl.when(inner & (t >= MID_LAG) & (t < n_sub + MID_LAG))
        def _():
            stage_mid(t - MID_LAG)

        @pl.when(jnp.logical_not(inner) & (t >= DOWN_LAG))
        def _():
            stage_down(t - DOWN_LAG)

    arrivals = ((x_hbm, x_s, x_snd, x_rcv), (dy_hbm, dy_s, dy_snd, dy_rcv))

    @pl.when(step == 0)
    def _():
        barrier = pltpu.get_barrier_semaphore()
        for d in OFFSETS:
            pl.semaphore_signal(barrier, inc=1, device_id=to(lax.rem(me + d, n_dev)), device_id_type=MESH)
        pl.semaphore_wait(barrier, n_dev - 1)
        for i in range(imgs):
            for src, dst, snd, rcv in arrivals:
                for d in OFFSETS:
                    scatter_in(src, dst, snd, rcv, i, d).start()
                local_in(src, dst, snd, i).start()
        for i in range(imgs):
            x_s[i, patches:] = xs_ref[i]
            dy_s[i, patches:] = dys_ref[i]
        vbuf[...] = jnp.zeros_like(vbuf)

    def receive(src, dst, snd, rcv, i):
        local_in(src, dst, snd, i).wait()
        for d in OFFSETS:
            scatter_in(src, dst, snd, rcv, i, d).wait_recv()

    def prepare(i):
        receive(*arrivals[0], i)

        def ln_body(t, carry):
            r = pl.ds(pl.multiple_of(t * chunk, 16), chunk)
            x_hat, _ = normalize(x_s[i, r])
            h_s[i, r] = (x_hat * ln_s[...] + ln_b[...]).astype(BF16)
            o_acc[i, r] = jnp.zeros((chunk, d_model), F32)
            dh_acc[i, r] = jnp.zeros((chunk, d_model), F32)
            return carry
        lax.fori_loop(0, CHUNK_TILES, ln_body, 0)
        receive(*arrivals[1], i)

        def dy_body(t, total):
            r = pl.ds(pl.multiple_of(t * chunk, 16), chunk)
            d_proj = dy_s[i, r].astype(F32) * l_scale[...]
            dp_s[i, r] = d_proj.astype(BF16)
            return total + jnp.sum(d_proj, axis=0, keepdims=True)
        d_bias = lax.fori_loop(0, CHUNK_TILES, dy_body, jnp.zeros((1, d_model), F32))
        for c in range(8):
            vbuf[40 + c:41 + c] += d_bias[:, c * LANES:(c + 1) * LANES]

    bias = jnp.concatenate([bq[...], bk[...], bv[...]], axis=1)
    for j, ref in enumerate((wq, wk, wv)):
        w_s[:, j * LANES:(j + 1) * LANES] = ref[...]

    lane = lax.broadcasted_iota(jnp.int32, (1, LANES), 1)
    zero = jnp.zeros((), BF16)

    def attend(i, carry):
        @pl.when((i == imgs - 1) & (step >= 1))
        def _():
            tick(SUBS * step - 2)

        @pl.when(step == 0)
        def _():
            prepare(i)

        qkv_s[i] = (dot_nn(h_s[i], w_s[...]) + bias).astype(BF16)
        da_s[i] = dot_nt(dp_s[i], wp[...]).astype(BF16)
        q, k, v = (qkv_s[i, :, j * LANES:(j + 1) * LANES] for j in range(3))
        da = da_s[i]
        a = jnp.zeros((rows, LANES), F32)
        dq, dk, dv = a, a, a
        keep_col = lax.broadcasted_iota(jnp.int32, (1, rows), 1) < patches + special
        for t in range(LANES // HEAD_DIM):
            mine = (lane // HEAD_DIM) == t
            qm, km, vm, dam = (jnp.where(mine, y, zero) for y in (q, k, v, da))
            s = dot_nt(qm, k) * ATTN_SCALE
            s = jnp.where(keep_col, s, NEG)
            e = jnp.exp(s - jnp.max(s, axis=-1, keepdims=True))
            p = e * (1.0 / jnp.sum(e, axis=-1, keepdims=True))
            p_lo = p.astype(BF16)
            a = a + dot_nn(p_lo, vm)
            dv = dv + dot_tn(p_lo, dam)
            dp = dot_nt(dam, v).astype(BF16).astype(F32)
            ds = (p * (dp - jnp.sum(dp * p, axis=-1, keepdims=True)) * ATTN_SCALE).astype(BF16)
            dq = dq + dot_nn(ds, km)
            dk = dk + dot_tn(ds, qm)
        a_s[i] = a.astype(BF16)
        for j, grad in enumerate((dq, dk, dv)):
            g_s[i, :, j * LANES:(j + 1) * LANES] = grad.astype(BF16)
        return carry
    lax.fori_loop(0, imgs, attend, 0)

    slot = lax.rem(step, 2)
    d_qkv = sum(jnp.sum(g_s[i].astype(F32), axis=0, keepdims=True) for i in range(imgs))
    for j in range(3):
        vbuf[pl.ds(j * 8 + step, 1)] = d_qkv[:, j * LANES:(j + 1) * LANES]

    def weight_grads(t, carry):
        c = pl.ds(pl.multiple_of(t * sub, sub), sub)
        dwb[slot, t, :, :3 * LANES] = sum(dot_tn(h_s[i, :, c], g_s[i]) for i in range(imgs))
        dwb[slot, t, :, 3 * LANES:] = sum(dot_tn(dp_s[i, :, c], a_s[i]) for i in range(imgs))
        return carry
    lax.fori_loop(0, 2 * SUBS, weight_grads, 0)

    pair_copy(step).start()

    def back(i, carry):
        o_acc[i] += dot_nn(a_s[i], wp[...])
        dh_acc[i] += dot_nt(g_s[i], w_s[...])
        return carry
    lax.fori_loop(0, imgs, back, 0)

    @pl.when(step >= 1)
    def _():
        tick(SUBS * step - 1)
    stage_pair(step)

    @pl.when(step == n_steps - 1)
    def _():
        def out_body(t, total):
            i, r = t // CHUNK_TILES, pl.multiple_of(lax.rem(t, CHUNK_TILES) * chunk, 16)
            proj = o_acc[i, pl.ds(r, chunk)] + b_proj[...]
            h_s[i, pl.ds(r, chunk)] = (x_s[i, pl.ds(r, chunk)].astype(F32) + l_scale[...] * proj).astype(BF16)
            return total + jnp.sum(dy_s[i, pl.ds(r, chunk)].astype(F32) * proj, axis=0, keepdims=True)
        d_scale = lax.fori_loop(0, imgs * CHUNK_TILES, out_body, jnp.zeros((1, d_model), F32))
        for d in OFFSETS:
            scatter_out(h_s, out_hbm, out_snd, out_rcv, d).start()
        local_out(h_s, out_hbm, loc.at[2]).start()

        tick(n_sub - 2)

        def dx_body(t, carry):
            t_scale, t_bias = carry
            i, r = t // CHUNK_TILES, pl.multiple_of(lax.rem(t, CHUNK_TILES) * chunk, 16)
            x_hat, inv = normalize(x_s[i, pl.ds(r, chunk)])
            grad = dh_acc[i, pl.ds(r, chunk)].astype(BF16).astype(F32)
            g_hat = grad * ln_s[...]
            d_row = inv * (g_hat - jnp.mean(g_hat, axis=-1, keepdims=True) - x_hat * jnp.mean(g_hat * x_hat, axis=-1, keepdims=True))
            dp_s[i, pl.ds(r, chunk)] = (dy_s[i, pl.ds(r, chunk)].astype(F32) + d_row).astype(BF16)
            return t_scale + jnp.sum(grad * x_hat, axis=0, keepdims=True), t_bias + jnp.sum(grad, axis=0, keepdims=True)
        none = jnp.zeros((1, d_model), F32)
        d_ln_s, d_ln_b = lax.fori_loop(0, imgs * CHUNK_TILES, dx_body, (none, none))
        tick(n_sub - 1)
        for d in OFFSETS:
            scatter_out(dp_s, dx_hbm, dx_snd, dx_rcv, d).start()
        local_out(dp_s, dx_hbm, loc.at[3]).start()

        for c in range(8):
            part = slice(c * LANES, (c + 1) * LANES)
            vbuf[24 + c:25 + c] = d_ln_s[:, part]
            vbuf[32 + c:33 + c] = d_ln_b[:, part]
            vbuf[48 + c:49 + c] = d_scale[:, part]
            for i in range(imgs):
                vbuf[56 + 8 * i + c:57 + 8 * i + c] = h_s[i, patches:, part].astype(F32)[:1]
                vbuf[72 + 8 * i + c:73 + 8 * i + c] = dp_s[i, patches:, part].astype(F32)[:1]
        for d in OFFSETS:
            vec_copy(d).start()
        pltpu.make_async_copy(vbuf, vec_hbm.at[me], loc.at[4]).start()

        for t in range(DOWN_LAG):
            tick(n_sub + t)

        local_out(h_s, out_hbm, loc.at[2]).wait()
        local_out(dp_s, dx_hbm, loc.at[3]).wait()
        pltpu.make_async_copy(vbuf, vec_hbm.at[me], loc.at[4]).wait()
        for d in OFFSETS:
            for i in range(imgs):
                for src, dst, snd, rcv in arrivals:
                    scatter_in(src, dst, snd, rcv, i, d).wait_send()
            scatter_out(h_s, out_hbm, out_snd, out_rcv, d).wait()
            scatter_out(dp_s, dx_hbm, dx_snd, dx_rcv, d).wait()
            vec_copy(d).wait()

        def drain(b, carry):
            up_copy(b).wait_send()

            @pl.when(inner)
            def _():
                mid_copy(b).wait_send()
            for copy in share_copies(b) + keep_copies(b):
                copy.wait()
            return carry
        lax.fori_loop(0, n_sub, drain, 0)


def solution(mesh):
    n_dev = mesh.shape['sp']

    def local_block(x_special, x_patch, dy_special, dy_patch, ln_scale, ln_bias, w_qkv, b_qkv, w_proj, b_proj, layer_scale):
        num_images, special, d_model = x_special.shape
        loc_p = x_patch.shape[1]
        imgs = num_images // n_dev
        pairs = d_model // LANES
        rows = n_dev * loc_p + PAD
        me = lax.axis_index('sp')

        def own_special(arr):
            own = lax.dynamic_slice_in_dim(arr, me * imgs, imgs, axis=0)
            return jnp.pad(own, ((0, 0), (0, PAD - special), (0, 0)))

        def whole(shape):
            return pl.BlockSpec(shape, lambda g: (0,) * len(shape))

        any_spec = pl.BlockSpec(memory_space=pl.ANY)
        row = (1, d_model)
        w_specs = [pl.BlockSpec((d_model, LANES), functools.partial(lambda j, g: (0, j * pairs + g), j)) for j in range(3)]
        b_specs = [pl.BlockSpec((1, LANES), functools.partial(lambda j, g: (0, j * pairs + g), j)) for j in range(3)]
        dma = pltpu.SemaphoreType.DMA
        big = (imgs, rows, d_model)
        thin = (imgs, rows, LANES)
        sub = d_model // (2 * SUBS)
        slots = pltpu.VMEM((SUBS * pairs, sub, 4 * LANES), F32)
        wide = (imgs, rows, 3 * LANES)
        out_p, dx_p, d_w_qkv, d_w_proj_t, vecs = pl.pallas_call(
            functools.partial(block_kernel, n_dev, special),
            grid=(pairs,),
            out_shape=(
                jax.ShapeDtypeStruct(x_patch.shape, BF16), jax.ShapeDtypeStruct(x_patch.shape, BF16),
                jax.ShapeDtypeStruct((d_model, 3 * d_model), F32), jax.ShapeDtypeStruct((d_model, d_model), F32), jax.ShapeDtypeStruct((n_dev, 88, LANES), F32)),
            in_specs=[any_spec, any_spec, whole((imgs, PAD, d_model)), whole((imgs, PAD, d_model)), whole(row), whole(row),
                      *w_specs, *b_specs, pl.BlockSpec((LANES, d_model), lambda g: (g, 0)), whole(row), whole(row)],
            out_specs=(any_spec,) * 5,
            scratch_shapes=[
                *[pltpu.VMEM(big, BF16)] * 4, *[pltpu.VMEM(big, F32)] * 2, pltpu.VMEM((d_model, 3 * LANES), BF16), *[pltpu.VMEM(wide, BF16)] * 2, *[pltpu.VMEM(thin, BF16)] * 2,
                pltpu.VMEM((2, 2 * SUBS, sub, 4 * LANES), F32), slots, slots, slots, pltpu.VMEM((88, LANES), F32),
                *[dma((imgs, n_dev))] * 4, *[dma((n_dev,))] * 6, *[dma((pairs,))] * 2, *[dma((SUBS * pairs,))] * 4, *[dma((SUBS * pairs, 4))] * 3, dma((5,))],
            compiler_params=pltpu.CompilerParams(
                collective_id=0, has_side_effects=True, dimension_semantics=('arbitrary',), vmem_limit_bytes=67_000_000),
        )(x_patch, dy_patch, own_special(x_special), own_special(dy_special), ln_scale[None], ln_bias[None],
          w_qkv, w_qkv, w_qkv, b_qkv[None], b_qkv[None], b_qkv[None], w_proj, b_proj[None], layer_scale[None])

        d_w_proj = d_w_proj_t.T
        sums = jnp.sum(vecs[:, :56], axis=0).reshape(7, d_model)
        lone = vecs[:, 56:].reshape(n_dev, 2, imgs, special, d_model).astype(BF16)
        out_s = lone[:, 0].reshape(x_special.shape)
        dx_s = lone[:, 1].reshape(x_special.shape)
        return (out_s, out_p, dx_s, dx_p, sums[3], sums[4], d_w_qkv, sums[:3].reshape(3 * d_model), d_w_proj, sums[5], sums[6])

    part_rows = P('dp')
    part_seq = P('dp', 'sp')
    replicated = P()
    return jax.shard_map(
        local_block, mesh=mesh,
        in_specs=(part_rows, part_seq, part_rows, part_seq, replicated, replicated, replicated, replicated, replicated, replicated, replicated),
        out_specs=(part_rows, part_seq, part_rows, part_seq, part_rows, part_rows, part_rows, part_rows, part_rows, part_rows, part_rows),
        check_vma=False)
```

```python
import functools

import jax
import jax.numpy as jnp
from jax import lax
from jax.experimental import pallas as pl
from jax.experimental.pallas import tpu as pltpu
from jax.sharding import PartitionSpec as P

HEAD_DIM = 64
LN_EPS = 1e-6
ATTN_SCALE = HEAD_DIM ** -0.5
LANES = 128
PAD = 16
CHUNK_TILES = 3
SUBS = 2
PIECES = 2
MID_LAG = 2
DOWN_LAG = 8
OFFSETS = (4, 3, 5, 2, 6, 1, 7)
MESH = pl.DeviceIdType.MESH
F32 = jnp.float32
BF16 = jnp.bfloat16
NEG = -1e30


def dot_nn(a, b):
    return lax.dot_general(a, b, (((1,), (0,)), ((), ())), preferred_element_type=F32)


def dot_nt(a, b):
    return lax.dot_general(a, b, (((1,), (1,)), ((), ())), preferred_element_type=F32)


def dot_tn(a, b):
    return lax.dot_general(a, b, (((0,), (0,)), ((), ())), preferred_element_type=F32)


def normalize(x):
    x = x.astype(F32)
    centered = x - jnp.mean(x, axis=-1, keepdims=True)
    inv = lax.rsqrt(jnp.mean(centered * centered, axis=-1, keepdims=True) + LN_EPS)
    return centered * inv, inv


def block_kernel(n_dev, special, x_hbm, dy_hbm, xs_ref, dys_ref, ln_s, ln_b, wq, wk, wv, bq, bk, bv, wp, b_proj, l_scale,
                 out_hbm, dx_hbm, dwq_hbm, dwp_hbm, vec_hbm,
                 x_s, dy_s, h_s, dp_s, o_acc, dh_acc, w_s, qkv_s, g_s, da_s, a_s, p_s, dwb, recv0, recv_a, recv_b, vbuf,
                 x_snd, x_rcv, dy_snd, dy_rcv, out_snd, out_rcv, dx_snd, dx_rcv, vec_snd, vec_rcv,
                 s0, r0, s_a, r_a, s_b, r_b, s_d, r_d, s_l, loc):
    step = pl.program_id(0)
    n_steps = pl.num_programs(0)
    me = lax.axis_index('sp')
    core = lax.rem(me, 2)
    chip = me // 2
    partner = me + 1 - 2 * core
    inner = (chip == 1) | (chip == 2)
    odd = lax.rem(chip, 2)
    near_a = me + 2 - 4 * odd
    near_b = lax.rem(me + 6 + 4 * odd, n_dev)
    imgs, rows, d_model = x_s.shape
    patches = rows - PAD
    loc_p = patches // n_dev
    sub = dwb.shape[2]
    n_sub = SUBS * n_steps
    chunk = rows // CHUNK_TILES

    def to(peer):
        return {'sp': peer}

    def remote(src, dst, snd, rcv, peer):
        return pltpu.make_async_remote_copy(src, dst, snd, rcv, device_id=to(peer), device_id_type=MESH)

    def scatter_in(src, dst, snd, rcv, i, d):
        peer = lax.rem(me + d, n_dev)
        return remote(src.at[peer * imgs + i], dst.at[i, pl.ds(pl.multiple_of(me * loc_p, loc_p), loc_p)], snd.at[i, d], rcv.at[i, d], peer)

    def local_in(src, dst, snd, i):
        return pltpu.make_async_copy(src.at[me * imgs + i], dst.at[i, pl.ds(pl.multiple_of(me * loc_p, loc_p), loc_p)], snd.at[i, 0])

    def scatter_out(src, dst, snd, rcv, d):
        peer = lax.rem(me + d, n_dev)
        return remote(src.at[:, pl.ds(pl.multiple_of(peer * loc_p, loc_p), loc_p)], dst.at[pl.ds(me * imgs, imgs)], snd.at[d], rcv.at[d], peer)

    def local_out(src, dst, sem):
        return pltpu.make_async_copy(src.at[:, pl.ds(pl.multiple_of(me * loc_p, loc_p), loc_p)], dst.at[pl.ds(me * imgs, imgs)], sem)

    def vec_copy(d):
        peer = lax.rem(me + d, n_dev)
        return remote(vbuf, vec_hbm.at[me], vec_snd.at[d], vec_rcv.at[d], peer)

    def pair_copy(g):
        return remote(dwb.at[lax.rem(g, 2), pl.ds(SUBS * (1 - core), SUBS)], recv0.at[pl.ds(SUBS * g, SUBS)], s0.at[g], r0.at[g], partner)

    def piece(h):
        return pl.ds(h * (sub // PIECES), sub // PIECES)

    def up_copy(b, h):
        return remote(recv0.at[b, piece(h)], recv_a.at[b, piece(h)], s_a.at[b, h], r_a.at[b, h], near_a)

    def mid_copy(b, h):
        return remote(recv0.at[b, piece(h)], recv_b.at[b, piece(h)], s_b.at[b, h], r_b.at[b, h], near_b)

    def down_copy(b):
        return remote(recv_a.at[b], recv_a.at[b], s_a.at[b, 0], r_a.at[b, 0], near_a)

    def results(b):
        r = pl.ds(pl.multiple_of((SUBS * core + lax.rem(b, SUBS)) * sub, sub), sub)
        col = (b // SUBS) * LANES
        for j in range(4):
            src = recv_a.at[b, :, pl.ds(j * LANES, LANES)]
            c = pl.ds(pl.multiple_of(col + (j * d_model if j < 3 else 0), LANES), LANES)
            yield j, src, (dwq_hbm if j < 3 else dwp_hbm).at[r, c]

    def share_copies(b):
        return [remote(src, dst, s_d.at[b, j], r_d.at[b, j], partner) for j, src, dst in results(b)]

    def keep_copies(b):
        return [pltpu.make_async_copy(src, dst, s_l.at[b, j]) for j, src, dst in results(b)]

    def publish(b):
        for copy in share_copies(b) + keep_copies(b):
            copy.start()

    parts = 2
    add_rows = sub // (PIECES * parts)

    def add_loop(h, add):
        def body(t, carry):
            add(pl.ds(pl.multiple_of(h * (sub // PIECES) + t * add_rows, add_rows), add_rows))
            return carry
        lax.fori_loop(0, parts, body, 0)

    def stage_pair(g):
        copy = pair_copy(g)
        copy.wait_recv()
        copy.wait_send()

        def one(t, carry):
            b = SUBS * g + t

            def add(r):
                recv0[b, r] += dwb[lax.rem(g, 2), SUBS * core + t, r]
            for h in range(PIECES):
                add_loop(h, add)

                @pl.when(jnp.logical_not(inner))
                def _():
                    up_copy(b, h).start()
            return carry
        lax.fori_loop(0, SUBS, one, 0)

    def stage_up(b):
        def add(r):
            recv0[b, r] += recv_a[b, r]
        for h in range(PIECES):
            up_copy(b, h).wait_recv()
            add_loop(h, add)
            mid_copy(b, h).start()

    def stage_mid(b):
        def add(r):
            recv_a[b, r] = recv0[b, r] + recv_b[b, r]
        for h in range(PIECES):
            mid_copy(b, h).wait_recv()
            add_loop(h, add)
        down_copy(b).start()
        publish(b)

    def stage_down(b):
        down_copy(b).wait_recv()
        publish(b)

    def tick(t):
        @pl.when(inner & (t < n_sub))
        def _():
            stage_up(t)

        @pl.when(inner & (t >= MID_LAG) & (t < n_sub + MID_LAG))
        def _():
            stage_mid(t - MID_LAG)

        @pl.when(jnp.logical_not(inner) & (t >= DOWN_LAG))
        def _():
            stage_down(t - DOWN_LAG)

    arrivals = ((x_hbm, x_s, x_snd, x_rcv), (dy_hbm, dy_s, dy_snd, dy_rcv))

    @pl.when(step == 0)
    def _():
        barrier = pltpu.get_barrier_semaphore()
        for d in OFFSETS:
            pl.semaphore_signal(barrier, inc=1, device_id=to(lax.rem(me + d, n_dev)), device_id_type=MESH)
        pl.semaphore_wait(barrier, n_dev - 1)
        for i in range(imgs):
            for src, dst, snd, rcv in arrivals:
                for d in OFFSETS:
                    scatter_in(src, dst, snd, rcv, i, d).start()
                local_in(src, dst, snd, i).start()
        for i in range(imgs):
            x_s[i, patches:] = xs_ref[i]
            dy_s[i, patches:] = dys_ref[i]
        vbuf[...] = jnp.zeros_like(vbuf)

    def receive(src, dst, snd, rcv, i):
        local_in(src, dst, snd, i).wait()
        for d in OFFSETS:
            scatter_in(src, dst, snd, rcv, i, d).wait_recv()

    def prepare_rows(i):
        receive(*arrivals[0], i)

        def ln_body(t, carry):
            r = pl.ds(pl.multiple_of(t * chunk, 16), chunk)
            x_hat, _ = normalize(x_s[i, r])
            h_s[i, r] = (x_hat * ln_s[...] + ln_b[...]).astype(BF16)
            o_acc[i, r] = jnp.zeros((chunk, d_model), F32)
            dh_acc[i, r] = jnp.zeros((chunk, d_model), F32)
            return carry
        lax.fori_loop(0, CHUNK_TILES, ln_body, 0)

    def prepare_back(i):
        receive(*arrivals[1], i)

        def dy_body(t, total):
            r = pl.ds(pl.multiple_of(t * chunk, 16), chunk)
            d_proj = dy_s[i, r].astype(F32) * l_scale[...]
            dp_s[i, r] = d_proj.astype(BF16)
            return total + jnp.sum(d_proj, axis=0, keepdims=True)
        d_bias = lax.fori_loop(0, CHUNK_TILES, dy_body, jnp.zeros((1, d_model), F32))
        for c in range(8):
            vbuf[40 + c:41 + c] += d_bias[:, c * LANES:(c + 1) * LANES]

    bias = jnp.concatenate([bq[...], bk[...], bv[...]], axis=1)
    for j, ref in enumerate((wq, wk, wv)):
        w_s[:, j * LANES:(j + 1) * LANES] = ref[...]

    lane = lax.broadcasted_iota(jnp.int32, (1, LANES), 1)
    zero = jnp.zeros((), BF16)

    def attend(i, carry):
        @pl.when((i == imgs - 1) & (step >= 1))
        def _():
            tick(SUBS * step - 2)

        @pl.when(step == 0)
        def _():
            prepare_rows(i)

        qkv_s[i] = (dot_nn(h_s[i], w_s[...]) + bias).astype(BF16)
        q, k, v = (qkv_s[i, :, j * LANES:(j + 1) * LANES] for j in range(3))
        a = jnp.zeros((rows, LANES), F32)
        dq, dk, dv = a, a, a
        keep_col = lax.broadcasted_iota(jnp.int32, (1, rows), 1) < patches + special
        heads = [(lane // HEAD_DIM) == t for t in range(LANES // HEAD_DIM)]
        for t, mine in enumerate(heads):
            s = dot_nt(jnp.where(mine, q, zero), k) * ATTN_SCALE
            s = jnp.where(keep_col, s, NEG)
            e = jnp.exp(s - jnp.max(s, axis=-1, keepdims=True))
            p = e * (1.0 / jnp.sum(e, axis=-1, keepdims=True))
            p_s[t] = p
            a = a + dot_nn(p.astype(BF16), jnp.where(mine, v, zero))

        @pl.when(step == 0)
        def _():
            prepare_back(i)

        da_s[i] = dot_nt(dp_s[i], wp[...]).astype(BF16)
        da = da_s[i]
        for t, mine in enumerate(heads):
            qm, km, dam = (jnp.where(mine, y, zero) for y in (q, k, da))
            p = p_s[t]
            dv = dv + dot_tn(p.astype(BF16), dam)
            dp = dot_nt(dam, v).astype(BF16).astype(F32)
            ds = (p * (dp - jnp.sum(dp * p, axis=-1, keepdims=True)) * ATTN_SCALE).astype(BF16)
            dq = dq + dot_nn(ds, km)
            dk = dk + dot_tn(ds, qm)
        a_s[i] = a.astype(BF16)
        for j, grad in enumerate((dq, dk, dv)):
            g_s[i, :, j * LANES:(j + 1) * LANES] = grad.astype(BF16)
        return carry
    lax.fori_loop(0, imgs, attend, 0)

    slot = lax.rem(step, 2)
    def weight_grads(n, carry):
        t = lax.rem(n + SUBS * (1 - core), 2 * SUBS)
        c = pl.ds(pl.multiple_of(t * sub, sub), sub)
        dwb[slot, t, :, :3 * LANES] = sum(dot_tn(h_s[i, :, c], g_s[i]) for i in range(imgs))
        dwb[slot, t, :, 3 * LANES:] = sum(dot_tn(dp_s[i, :, c], a_s[i]) for i in range(imgs))
        return carry
    lax.fori_loop(0, SUBS, weight_grads, 0)
    pair_copy(step).start()
    lax.fori_loop(SUBS, 2 * SUBS, weight_grads, 0)

    d_qkv = sum(jnp.sum(g_s[i].astype(F32), axis=0, keepdims=True) for i in range(imgs))
    for j in range(3):
        vbuf[pl.ds(j * 8 + step, 1)] = d_qkv[:, j * LANES:(j + 1) * LANES]


    def back(i, carry):
        o_acc[i] += dot_nn(a_s[i], wp[...])
        dh_acc[i] += dot_nt(g_s[i], w_s[...])
        return carry
    lax.fori_loop(0, imgs, back, 0)

    @pl.when(step >= 1)
    def _():
        tick(SUBS * step - 1)
    stage_pair(step)

    @pl.when(step == n_steps - 1)
    def _():
        def out_body(t, total):
            i, r = t // CHUNK_TILES, pl.multiple_of(lax.rem(t, CHUNK_TILES) * chunk, 16)
            proj = o_acc[i, pl.ds(r, chunk)] + b_proj[...]
            h_s[i, pl.ds(r, chunk)] = (x_s[i, pl.ds(r, chunk)].astype(F32) + l_scale[...] * proj).astype(BF16)
            return total + jnp.sum(dy_s[i, pl.ds(r, chunk)].astype(F32) * proj, axis=0, keepdims=True)
        d_scale = lax.fori_loop(0, imgs * CHUNK_TILES, out_body, jnp.zeros((1, d_model), F32))
        for d in OFFSETS:
            scatter_out(h_s, out_hbm, out_snd, out_rcv, d).start()
        local_out(h_s, out_hbm, loc.at[2]).start()

        tick(n_sub - 2)

        def dx_body(t, carry):
            t_scale, t_bias = carry
            i, r = t // CHUNK_TILES, pl.multiple_of(lax.rem(t, CHUNK_TILES) * chunk, 16)
            x_hat, inv = normalize(x_s[i, pl.ds(r, chunk)])
            grad = dh_acc[i, pl.ds(r, chunk)].astype(BF16).astype(F32)
            g_hat = grad * ln_s[...]
            d_row = inv * (g_hat - jnp.mean(g_hat, axis=-1, keepdims=True) - x_hat * jnp.mean(g_hat * x_hat, axis=-1, keepdims=True))
            dp_s[i, pl.ds(r, chunk)] = (dy_s[i, pl.ds(r, chunk)].astype(F32) + d_row).astype(BF16)
            return t_scale + jnp.sum(grad * x_hat, axis=0, keepdims=True), t_bias + jnp.sum(grad, axis=0, keepdims=True)
        none = jnp.zeros((1, d_model), F32)
        d_ln_s, d_ln_b = lax.fori_loop(0, imgs * CHUNK_TILES, dx_body, (none, none))
        tick(n_sub - 1)
        for d in OFFSETS:
            scatter_out(dp_s, dx_hbm, dx_snd, dx_rcv, d).start()
        local_out(dp_s, dx_hbm, loc.at[3]).start()

        for c in range(8):
            part = slice(c * LANES, (c + 1) * LANES)
            vbuf[24 + c:25 + c] = d_ln_s[:, part]
            vbuf[32 + c:33 + c] = d_ln_b[:, part]
            vbuf[48 + c:49 + c] = d_scale[:, part]
            for i in range(imgs):
                vbuf[56 + 8 * i + c:57 + 8 * i + c] = h_s[i, patches:, part].astype(F32)[:1]
                vbuf[72 + 8 * i + c:73 + 8 * i + c] = dp_s[i, patches:, part].astype(F32)[:1]
        for d in OFFSETS:
            vec_copy(d).start()
        pltpu.make_async_copy(vbuf, vec_hbm.at[me], loc.at[4]).start()

        for t in range(DOWN_LAG):
            tick(n_sub + t)

        local_out(h_s, out_hbm, loc.at[2]).wait()
        local_out(dp_s, dx_hbm, loc.at[3]).wait()
        pltpu.make_async_copy(vbuf, vec_hbm.at[me], loc.at[4]).wait()
        for d in OFFSETS:
            for i in range(imgs):
                for src, dst, snd, rcv in arrivals:
                    scatter_in(src, dst, snd, rcv, i, d).wait_send()
            scatter_out(h_s, out_hbm, out_snd, out_rcv, d).wait()
            scatter_out(dp_s, dx_hbm, dx_snd, dx_rcv, d).wait()
            vec_copy(d).wait()

        def drain(b, carry):
            @pl.when(inner)
            def _():
                down_copy(b).wait_send()
                for h in range(PIECES):
                    mid_copy(b, h).wait_send()

            @pl.when(jnp.logical_not(inner))
            def _():
                for h in range(PIECES):
                    up_copy(b, h).wait_send()
            for copy in share_copies(b) + keep_copies(b):
                copy.wait()
            return carry
        lax.fori_loop(0, n_sub, drain, 0)


def solution(mesh):
    n_dev = mesh.shape['sp']

    def local_block(x_special, x_patch, dy_special, dy_patch, ln_scale, ln_bias, w_qkv, b_qkv, w_proj, b_proj, layer_scale):
        num_images, special, d_model = x_special.shape
        loc_p = x_patch.shape[1]
        imgs = num_images // n_dev
        pairs = d_model // LANES
        rows = n_dev * loc_p + PAD
        me = lax.axis_index('sp')

        def own_special(arr):
            own = lax.dynamic_slice_in_dim(arr, me * imgs, imgs, axis=0)
            return jnp.pad(own, ((0, 0), (0, PAD - special), (0, 0)))

        def whole(shape):
            return pl.BlockSpec(shape, lambda g: (0,) * len(shape))

        any_spec = pl.BlockSpec(memory_space=pl.ANY)
        row = (1, d_model)
        w_specs = [pl.BlockSpec((d_model, LANES), functools.partial(lambda j, g: (0, j * pairs + g), j)) for j in range(3)]
        b_specs = [pl.BlockSpec((1, LANES), functools.partial(lambda j, g: (0, j * pairs + g), j)) for j in range(3)]
        dma = pltpu.SemaphoreType.DMA
        big = (imgs, rows, d_model)
        thin = (imgs, rows, LANES)
        sub = d_model // (2 * SUBS)
        slots = pltpu.VMEM((SUBS * pairs, sub, 4 * LANES), F32)
        wide = (imgs, rows, 3 * LANES)
        out_p, dx_p, d_w_qkv, d_w_proj_t, vecs = pl.pallas_call(
            functools.partial(block_kernel, n_dev, special),
            grid=(pairs,),
            out_shape=(
                jax.ShapeDtypeStruct(x_patch.shape, BF16), jax.ShapeDtypeStruct(x_patch.shape, BF16),
                jax.ShapeDtypeStruct((d_model, 3 * d_model), F32), jax.ShapeDtypeStruct((d_model, d_model), F32), jax.ShapeDtypeStruct((n_dev, 88, LANES), F32)),
            in_specs=[any_spec, any_spec, whole((imgs, PAD, d_model)), whole((imgs, PAD, d_model)), whole(row), whole(row),
                      *w_specs, *b_specs, pl.BlockSpec((LANES, d_model), lambda g: (g, 0)), whole(row), whole(row)],
            out_specs=(any_spec,) * 5,
            scratch_shapes=[
                *[pltpu.VMEM(big, BF16)] * 4, *[pltpu.VMEM(big, F32)] * 2, pltpu.VMEM((d_model, 3 * LANES), BF16), *[pltpu.VMEM(wide, BF16)] * 2, *[pltpu.VMEM(thin, BF16)] * 2, pltpu.VMEM((LANES // HEAD_DIM, rows, rows), F32),
                pltpu.VMEM((2, 2 * SUBS, sub, 4 * LANES), F32), slots, slots, slots, pltpu.VMEM((88, LANES), F32),
                *[dma((imgs, n_dev))] * 4, *[dma((n_dev,))] * 6, *[dma((pairs,))] * 2, *[dma((SUBS * pairs, PIECES))] * 4, *[dma((SUBS * pairs, 4))] * 3, dma((5,))],
            compiler_params=pltpu.CompilerParams(
                collective_id=0, has_side_effects=True, dimension_semantics=('arbitrary',), vmem_limit_bytes=67_000_000),
        )(x_patch, dy_patch, own_special(x_special), own_special(dy_special), ln_scale[None], ln_bias[None],
          w_qkv, w_qkv, w_qkv, b_qkv[None], b_qkv[None], b_qkv[None], w_proj, b_proj[None], layer_scale[None])

        d_w_proj = d_w_proj_t.T
        sums = jnp.sum(vecs[:, :56], axis=0).reshape(7, d_model)
        lone = vecs[:, 56:].reshape(n_dev, 2, imgs, special, d_model).astype(BF16)
        out_s = lone[:, 0].reshape(x_special.shape)
        dx_s = lone[:, 1].reshape(x_special.shape)
        return (out_s, out_p, dx_s, dx_p, sums[3], sums[4], d_w_qkv, sums[:3].reshape(3 * d_model), d_w_proj, sums[5], sums[6])

    part_rows = P('dp')
    part_seq = P('dp', 'sp')
    replicated = P()
    return jax.shard_map(
        local_block, mesh=mesh,
        in_specs=(part_rows, part_seq, part_rows, part_seq, replicated, replicated, replicated, replicated, replicated, replicated, replicated),
        out_specs=(part_rows, part_seq, part_rows, part_seq, part_rows, part_rows, part_rows, part_rows, part_rows, part_rows, part_rows),
        check_vma=False)
```

```python
import functools

import jax
import jax.numpy as jnp
from jax import lax
from jax.experimental import pallas as pl
from jax.experimental.pallas import tpu as pltpu
from jax.sharding import PartitionSpec as P

HEAD_DIM = 64
LN_EPS = 1e-6
ATTN_SCALE = HEAD_DIM ** -0.5
LANES = 128
PAD = 16
CHUNK_TILES = 3
SUBS = 2
PIECES = 2
MID_LAG = 3
DOWN_LAG = 8
OFFSETS = (4, 3, 5, 2, 6, 1, 7)
MESH = pl.DeviceIdType.MESH
F32 = jnp.float32
BF16 = jnp.bfloat16
NEG = -1e30


def dot_nn(a, b):
    return lax.dot_general(a, b, (((1,), (0,)), ((), ())), preferred_element_type=F32)


def dot_nt(a, b):
    return lax.dot_general(a, b, (((1,), (1,)), ((), ())), preferred_element_type=F32)


def dot_tn(a, b):
    return lax.dot_general(a, b, (((0,), (0,)), ((), ())), preferred_element_type=F32)


def normalize(x):
    x = x.astype(F32)
    centered = x - jnp.mean(x, axis=-1, keepdims=True)
    inv = lax.rsqrt(jnp.mean(centered * centered, axis=-1, keepdims=True) + LN_EPS)
    return centered * inv, inv


def block_kernel(n_dev, special, x_hbm, dy_hbm, xs_ref, dys_ref, ln_s, ln_b, wq, wk, wv, bq, bk, bv, wp, b_proj, l_scale,
                 out_hbm, dx_hbm, dwq_hbm, dwp_hbm, vec_hbm,
                 x_s, dy_s, h_s, dp_s, o_acc, dh_acc, w_s, qkv_s, g_s, da_s, a_s, p_s, dwb, recv0, recv_a, recv_b, vbuf,
                 x_snd, x_rcv, dy_snd, dy_rcv, out_snd, out_rcv, dx_snd, dx_rcv, vec_snd, vec_rcv,
                 s0, r0, s_a, r_a, s_b, r_b, s_d, r_d, s_l, loc):
    step = pl.program_id(0)
    n_steps = pl.num_programs(0)
    me = lax.axis_index('sp')
    core = lax.rem(me, 2)
    chip = me // 2
    partner = me + 1 - 2 * core
    inner = (chip == 1) | (chip == 2)
    odd = lax.rem(chip, 2)
    near_a = me + 2 - 4 * odd
    near_b = lax.rem(me + 6 + 4 * odd, n_dev)
    imgs, rows, d_model = x_s.shape
    patches = rows - PAD
    loc_p = patches // n_dev
    sub = dwb.shape[2]
    n_sub = SUBS * n_steps
    chunk = rows // CHUNK_TILES

    def to(peer):
        return {'sp': peer}

    def remote(src, dst, snd, rcv, peer):
        return pltpu.make_async_remote_copy(src, dst, snd, rcv, device_id=to(peer), device_id_type=MESH)

    def scatter_in(src, dst, snd, rcv, i, d):
        peer = lax.rem(me + d, n_dev)
        return remote(src.at[peer * imgs + i], dst.at[i, pl.ds(pl.multiple_of(me * loc_p, loc_p), loc_p)], snd.at[i, d], rcv.at[i, d], peer)

    def local_in(src, dst, snd, i):
        return pltpu.make_async_copy(src.at[me * imgs + i], dst.at[i, pl.ds(pl.multiple_of(me * loc_p, loc_p), loc_p)], snd.at[i, 0])

    def scatter_out(src, dst, snd, rcv, d):
        peer = lax.rem(me + d, n_dev)
        return remote(src.at[:, pl.ds(pl.multiple_of(peer * loc_p, loc_p), loc_p)], dst.at[pl.ds(me * imgs, imgs)], snd.at[d], rcv.at[d], peer)

    def local_out(src, dst, sem):
        return pltpu.make_async_copy(src.at[:, pl.ds(pl.multiple_of(me * loc_p, loc_p), loc_p)], dst.at[pl.ds(me * imgs, imgs)], sem)

    def vec_copy(d):
        peer = lax.rem(me + d, n_dev)
        return remote(vbuf, vec_hbm.at[me], vec_snd.at[d], vec_rcv.at[d], peer)

    def pair_copy(g):
        return remote(dwb.at[lax.rem(g, 2), pl.ds(SUBS * (1 - core), SUBS)], recv0.at[pl.ds(SUBS * g, SUBS)], s0.at[g], r0.at[g], partner)

    def piece(h):
        return pl.ds(h * (sub // PIECES), sub // PIECES)

    def up_copy(b, h):
        return remote(recv0.at[b, piece(h)], recv_a.at[b, piece(h)], s_a.at[b, h], r_a.at[b, h], near_a)

    def mid_copy(b, h):
        return remote(recv0.at[b, piece(h)], recv_b.at[b, piece(h)], s_b.at[b, h], r_b.at[b, h], near_b)

    def down_copy(b):
        return remote(recv_a.at[b], recv_a.at[b], s_a.at[b, 0], r_a.at[b, 0], near_a)

    def results(b):
        r = pl.ds(pl.multiple_of((SUBS * core + lax.rem(b, SUBS)) * sub, sub), sub)
        col = (b // SUBS) * LANES
        for j in range(4):
            src = recv_a.at[b, :, pl.ds(j * LANES, LANES)]
            c = pl.ds(pl.multiple_of(col + (j * d_model if j < 3 else 0), LANES), LANES)
            yield j, src, (dwq_hbm if j < 3 else dwp_hbm).at[r, c]

    def share_copies(b):
        return [remote(src, dst, s_d.at[b, j], r_d.at[b, j], partner) for j, src, dst in results(b)]

    def keep_copies(b):
        return [pltpu.make_async_copy(src, dst, s_l.at[b, j]) for j, src, dst in results(b)]

    def publish(b):
        for copy in share_copies(b) + keep_copies(b):
            copy.start()

    parts = 2
    add_rows = sub // (PIECES * parts)

    def add_loop(h, add):
        def body(t, carry):
            add(pl.ds(pl.multiple_of(h * (sub // PIECES) + t * add_rows, add_rows), add_rows))
            return carry
        lax.fori_loop(0, parts, body, 0)

    def stage_pair(g):
        copy = pair_copy(g)
        copy.wait_recv()
        copy.wait_send()

        def one(t, carry):
            b = SUBS * g + t

            def add(r):
                recv0[b, r] += dwb[lax.rem(g, 2), SUBS * core + t, r]
            for h in range(PIECES):
                add_loop(h, add)

                @pl.when(jnp.logical_not(inner))
                def _():
                    up_copy(b, h).start()
            return carry
        lax.fori_loop(0, SUBS, one, 0)

    def stage_up(b):
        def add(r):
            recv0[b, r] += recv_a[b, r]
        for h in range(PIECES):
            up_copy(b, h).wait_recv()
            add_loop(h, add)
            mid_copy(b, h).start()

    def stage_mid(b):
        def add(r):
            recv_a[b, r] = recv0[b, r] + recv_b[b, r]
        for h in range(PIECES):
            mid_copy(b, h).wait_recv()
            add_loop(h, add)
        down_copy(b).start()
        publish(b)

    def stage_down(b):
        down_copy(b).wait_recv()
        publish(b)

    def tick(t):
        @pl.when(inner & (t < n_sub))
        def _():
            stage_up(t)

        @pl.when(inner & (t >= MID_LAG) & (t < n_sub + MID_LAG))
        def _():
            stage_mid(t - MID_LAG)

        @pl.when(jnp.logical_not(inner) & (t >= DOWN_LAG))
        def _():
            stage_down(t - DOWN_LAG)

    arrivals = ((x_hbm, x_s, x_snd, x_rcv), (dy_hbm, dy_s, dy_snd, dy_rcv))

    @pl.when(step == 0)
    def _():
        barrier = pltpu.get_barrier_semaphore()
        for d in OFFSETS:
            pl.semaphore_signal(barrier, inc=1, device_id=to(lax.rem(me + d, n_dev)), device_id_type=MESH)
        pl.semaphore_wait(barrier, n_dev - 1)
        for i in range(imgs):
            for src, dst, snd, rcv in arrivals:
                for d in OFFSETS:
                    scatter_in(src, dst, snd, rcv, i, d).start()
                local_in(src, dst, snd, i).start()
        for i in range(imgs):
            x_s[i, patches:] = xs_ref[i]
            dy_s[i, patches:] = dys_ref[i]
        vbuf[...] = jnp.zeros_like(vbuf)

    def receive(src, dst, snd, rcv, i):
        local_in(src, dst, snd, i).wait()
        for d in OFFSETS:
            scatter_in(src, dst, snd, rcv, i, d).wait_recv()

    def prepare_rows(i):
        receive(*arrivals[0], i)

        def ln_body(t, carry):
            r = pl.ds(pl.multiple_of(t * chunk, 16), chunk)
            x_hat, _ = normalize(x_s[i, r])
            h_s[i, r] = (x_hat * ln_s[...] + ln_b[...]).astype(BF16)
            o_acc[i, r] = jnp.zeros((chunk, d_model), F32)
            dh_acc[i, r] = jnp.zeros((chunk, d_model), F32)
            return carry
        lax.fori_loop(0, CHUNK_TILES, ln_body, 0)

    def prepare_back(i):
        receive(*arrivals[1], i)

        def dy_body(t, total):
            r = pl.ds(pl.multiple_of(t * chunk, 16), chunk)
            d_proj = dy_s[i, r].astype(F32) * l_scale[...]
            dp_s[i, r] = d_proj.astype(BF16)
            return total + jnp.sum(d_proj, axis=0, keepdims=True)
        d_bias = lax.fori_loop(0, CHUNK_TILES, dy_body, jnp.zeros((1, d_model), F32))
        for c in range(8):
            vbuf[40 + c:41 + c] += d_bias[:, c * LANES:(c + 1) * LANES]

    bias = jnp.concatenate([bq[...], bk[...], bv[...]], axis=1)
    for j, ref in enumerate((wq, wk, wv)):
        w_s[:, j * LANES:(j + 1) * LANES] = ref[...]

    lane = lax.broadcasted_iota(jnp.int32, (1, LANES), 1)
    zero = jnp.zeros((), BF16)

    def attend(i, carry):
        @pl.when((i == imgs - 1) & (step >= 1))
        def _():
            tick(SUBS * step - 2)

        @pl.when(step == 0)
        def _():
            prepare_rows(i)

        qkv_s[i] = (dot_nn(h_s[i], w_s[...]) + bias).astype(BF16)
        q, k, v = (qkv_s[i, :, j * LANES:(j + 1) * LANES] for j in range(3))
        a = jnp.zeros((rows, LANES), F32)
        dq, dk, dv = a, a, a
        keep_col = lax.broadcasted_iota(jnp.int32, (1, rows), 1) < patches + special
        heads = [(lane // HEAD_DIM) == t for t in range(LANES // HEAD_DIM)]
        for t, mine in enumerate(heads):
            s = dot_nt(jnp.where(mine, q, zero), k) * ATTN_SCALE
            s = jnp.where(keep_col, s, NEG)
            e = jnp.exp(s - jnp.max(s, axis=-1, keepdims=True))
            p = e * (1.0 / jnp.sum(e, axis=-1, keepdims=True))
            p_s[t] = p
            a = a + dot_nn(p.astype(BF16), jnp.where(mine, v, zero))

        @pl.when(step == 0)
        def _():
            prepare_back(i)

        da_s[i] = dot_nt(dp_s[i], wp[...]).astype(BF16)
        da = da_s[i]
        for t, mine in enumerate(heads):
            qm, km, dam = (jnp.where(mine, y, zero) for y in (q, k, da))
            p = p_s[t]
            dv = dv + dot_tn(p.astype(BF16), dam)
            dp = dot_nt(dam, v).astype(BF16).astype(F32)
            ds = (p * (dp - jnp.sum(dp * p, axis=-1, keepdims=True)) * ATTN_SCALE).astype(BF16)
            dq = dq + dot_nn(ds, km)
            dk = dk + dot_tn(ds, qm)
        a_s[i] = a.astype(BF16)
        for j, grad in enumerate((dq, dk, dv)):
            g_s[i, :, j * LANES:(j + 1) * LANES] = grad.astype(BF16)
        return carry
    lax.fori_loop(0, imgs, attend, 0)

    slot = lax.rem(step, 2)
    def weight_grads(n, carry):
        t = lax.rem(n + SUBS * (1 - core), 2 * SUBS)
        c = pl.ds(pl.multiple_of(t * sub, sub), sub)
        dwb[slot, t, :, :3 * LANES] = sum(dot_tn(h_s[i, :, c], g_s[i]) for i in range(imgs))
        dwb[slot, t, :, 3 * LANES:] = sum(dot_tn(dp_s[i, :, c], a_s[i]) for i in range(imgs))
        return carry
    lax.fori_loop(0, SUBS, weight_grads, 0)
    pair_copy(step).start()
    lax.fori_loop(SUBS, 2 * SUBS, weight_grads, 0)

    d_qkv = sum(jnp.sum(g_s[i].astype(F32), axis=0, keepdims=True) for i in range(imgs))
    for j in range(3):
        vbuf[pl.ds(j * 8 + step, 1)] = d_qkv[:, j * LANES:(j + 1) * LANES]


    def back(i, carry):
        o_acc[i] += dot_nn(a_s[i], wp[...])
        dh_acc[i] += dot_nt(g_s[i], w_s[...])
        return carry
    lax.fori_loop(0, imgs, back, 0)

    stage_pair(step)

    @pl.when(step >= 1)
    def _():
        tick(SUBS * step - 1)

    @pl.when(step == n_steps - 1)
    def _():
        def out_body(t, total):
            i, r = t // CHUNK_TILES, pl.multiple_of(lax.rem(t, CHUNK_TILES) * chunk, 16)
            proj = o_acc[i, pl.ds(r, chunk)] + b_proj[...]
            h_s[i, pl.ds(r, chunk)] = (x_s[i, pl.ds(r, chunk)].astype(F32) + l_scale[...] * proj).astype(BF16)
            return total + jnp.sum(dy_s[i, pl.ds(r, chunk)].astype(F32) * proj, axis=0, keepdims=True)
        d_scale = lax.fori_loop(0, imgs * CHUNK_TILES, out_body, jnp.zeros((1, d_model), F32))
        for d in OFFSETS:
            scatter_out(h_s, out_hbm, out_snd, out_rcv, d).start()
        local_out(h_s, out_hbm, loc.at[2]).start()

        tick(n_sub - 2)

        def dx_body(t, carry):
            t_scale, t_bias = carry
            i, r = t // CHUNK_TILES, pl.multiple_of(lax.rem(t, CHUNK_TILES) * chunk, 16)
            x_hat, inv = normalize(x_s[i, pl.ds(r, chunk)])
            grad = dh_acc[i, pl.ds(r, chunk)].astype(BF16).astype(F32)
            g_hat = grad * ln_s[...]
            d_row = inv * (g_hat - jnp.mean(g_hat, axis=-1, keepdims=True) - x_hat * jnp.mean(g_hat * x_hat, axis=-1, keepdims=True))
            dp_s[i, pl.ds(r, chunk)] = (dy_s[i, pl.ds(r, chunk)].astype(F32) + d_row).astype(BF16)
            return t_scale + jnp.sum(grad * x_hat, axis=0, keepdims=True), t_bias + jnp.sum(grad, axis=0, keepdims=True)
        none = jnp.zeros((1, d_model), F32)
        d_ln_s, d_ln_b = lax.fori_loop(0, imgs * CHUNK_TILES, dx_body, (none, none))

        for c in range(8):
            part = slice(c * LANES, (c + 1) * LANES)
            vbuf[24 + c:25 + c] = d_ln_s[:, part]
            vbuf[32 + c:33 + c] = d_ln_b[:, part]
            vbuf[48 + c:49 + c] = d_scale[:, part]
            for i in range(imgs):
                vbuf[56 + 8 * i + c:57 + 8 * i + c] = h_s[i, patches:, part].astype(F32)[:1]
                vbuf[72 + 8 * i + c:73 + 8 * i + c] = dp_s[i, patches:, part].astype(F32)[:1]
        for d in OFFSETS:
            vec_copy(d).start()
        pltpu.make_async_copy(vbuf, vec_hbm.at[me], loc.at[4]).start()
        tick(n_sub - 1)
        for d in OFFSETS:
            scatter_out(dp_s, dx_hbm, dx_snd, dx_rcv, d).start()
        local_out(dp_s, dx_hbm, loc.at[3]).start()

        for t in range(DOWN_LAG):
            tick(n_sub + t)

        local_out(h_s, out_hbm, loc.at[2]).wait()
        local_out(dp_s, dx_hbm, loc.at[3]).wait()
        pltpu.make_async_copy(vbuf, vec_hbm.at[me], loc.at[4]).wait()
        for d in OFFSETS:
            for i in range(imgs):
                for src, dst, snd, rcv in arrivals:
                    scatter_in(src, dst, snd, rcv, i, d).wait_send()
            scatter_out(h_s, out_hbm, out_snd, out_rcv, d).wait()
            scatter_out(dp_s, dx_hbm, dx_snd, dx_rcv, d).wait()
            vec_copy(d).wait()

        def drain(b, carry):
            @pl.when(inner)
            def _():
                down_copy(b).wait_send()
                for h in range(PIECES):
                    mid_copy(b, h).wait_send()

            @pl.when(jnp.logical_not(inner))
            def _():
                for h in range(PIECES):
                    up_copy(b, h).wait_send()
            for copy in share_copies(b) + keep_copies(b):
                copy.wait()
            return carry
        lax.fori_loop(0, n_sub, drain, 0)


def solution(mesh):
    n_dev = mesh.shape['sp']

    def local_block(x_special, x_patch, dy_special, dy_patch, ln_scale, ln_bias, w_qkv, b_qkv, w_proj, b_proj, layer_scale):
        num_images, special, d_model = x_special.shape
        loc_p = x_patch.shape[1]
        imgs = num_images // n_dev
        pairs = d_model // LANES
        rows = n_dev * loc_p + PAD
        me = lax.axis_index('sp')

        def own_special(arr):
            own = lax.dynamic_slice_in_dim(arr, me * imgs, imgs, axis=0)
            return jnp.pad(own, ((0, 0), (0, PAD - special), (0, 0)))

        def whole(shape):
            return pl.BlockSpec(shape, lambda g: (0,) * len(shape))

        any_spec = pl.BlockSpec(memory_space=pl.ANY)
        row = (1, d_model)
        w_specs = [pl.BlockSpec((d_model, LANES), functools.partial(lambda j, g: (0, j * pairs + g), j)) for j in range(3)]
        b_specs = [pl.BlockSpec((1, LANES), functools.partial(lambda j, g: (0, j * pairs + g), j)) for j in range(3)]
        dma = pltpu.SemaphoreType.DMA
        big = (imgs, rows, d_model)
        thin = (imgs, rows, LANES)
        sub = d_model // (2 * SUBS)
        slots = pltpu.VMEM((SUBS * pairs, sub, 4 * LANES), F32)
        wide = (imgs, rows, 3 * LANES)
        out_p, dx_p, d_w_qkv, d_w_proj_t, vecs = pl.pallas_call(
            functools.partial(block_kernel, n_dev, special),
            grid=(pairs,),
            out_shape=(
                jax.ShapeDtypeStruct(x_patch.shape, BF16), jax.ShapeDtypeStruct(x_patch.shape, BF16),
                jax.ShapeDtypeStruct((d_model, 3 * d_model), F32), jax.ShapeDtypeStruct((d_model, d_model), F32), jax.ShapeDtypeStruct((n_dev, 88, LANES), F32)),
            in_specs=[any_spec, any_spec, whole((imgs, PAD, d_model)), whole((imgs, PAD, d_model)), whole(row), whole(row),
                      *w_specs, *b_specs, pl.BlockSpec((LANES, d_model), lambda g: (g, 0)), whole(row), whole(row)],
            out_specs=(any_spec,) * 5,
            scratch_shapes=[
                *[pltpu.VMEM(big, BF16)] * 4, *[pltpu.VMEM(big, F32)] * 2, pltpu.VMEM((d_model, 3 * LANES), BF16), *[pltpu.VMEM(wide, BF16)] * 2, *[pltpu.VMEM(thin, BF16)] * 2, pltpu.VMEM((LANES // HEAD_DIM, rows, rows), F32),
                pltpu.VMEM((2, 2 * SUBS, sub, 4 * LANES), F32), slots, slots, slots, pltpu.VMEM((88, LANES), F32),
                *[dma((imgs, n_dev))] * 4, *[dma((n_dev,))] * 6, *[dma((pairs,))] * 2, *[dma((SUBS * pairs, PIECES))] * 4, *[dma((SUBS * pairs, 4))] * 3, dma((5,))],
            compiler_params=pltpu.CompilerParams(
                collective_id=0, has_side_effects=True, dimension_semantics=('arbitrary',), vmem_limit_bytes=67_000_000),
        )(x_patch, dy_patch, own_special(x_special), own_special(dy_special), ln_scale[None], ln_bias[None],
          w_qkv, w_qkv, w_qkv, b_qkv[None], b_qkv[None], b_qkv[None], w_proj, b_proj[None], layer_scale[None])

        d_w_proj = d_w_proj_t.T
        sums = jnp.sum(vecs[:, :56], axis=0).reshape(7, d_model)
        lone = vecs[:, 56:].reshape(n_dev, 2, imgs, special, d_model).astype(BF16)
        out_s = lone[:, 0].reshape(x_special.shape)
        dx_s = lone[:, 1].reshape(x_special.shape)
        return (out_s, out_p, dx_s, dx_p, sums[3], sums[4], d_w_qkv, sums[:3].reshape(3 * d_model), d_w_proj, sums[5], sums[6])

    part_rows = P('dp')
    part_seq = P('dp', 'sp')
    replicated = P()
    return jax.shard_map(
        local_block, mesh=mesh,
        in_specs=(part_rows, part_seq, part_rows, part_seq, replicated, replicated, replicated, replicated, replicated, replicated, replicated),
        out_specs=(part_rows, part_seq, part_rows, part_seq, part_rows, part_rows, part_rows, part_rows, part_rows, part_rows, part_rows),
        check_vma=False)
```
